32 devices in a mesh: cells: 8 (over z, x), genes: 4 (over y, core).
Axes of the slice: x: 2, y: 2, z: 4, core: 2. Of those that a mesh axis runs over, the one named last changes fastest.
Arguments:
- counts: int32 [38912, 4000], P('cells', 'genes'), may hold values from 0 to 674, as said below
- sketch: bfloat16 [4000, 128], P('genes'), may hold values from -6 to 6
Outputs:
- basis: float32 [38912, 128], P('cells')
- loadings: float32 [4000, 128], P('genes')
The draws below stay inside these ranges and needn't reach their ends.
Inputs may be any that keep to these rules, and one draw needn't show every extreme that they name: `counts`: every cell and every gene has a positive total.
All inputs are finite; a program needn't handle non-finite values.
Results may differ from the reference program's by a relative error of at most 0.0051.
Values may be sent and summed in bfloat16 or wider, within the bound.
A program may use at most 128 MiB of HBM per device.

```python
import math
import jax
import jax.numpy as jnp
from jax import lax

CELL_DEV = 4864
GENES = 4000
RANK = 128
ITERS = 2
CELLS = 38912
N_CELLS = 8


def draw_counts(key, part):
    subkeys = jax.random.split(key, 4)
    row_ids = jnp.arange(CELLS, dtype=jnp.int32)[:, None]
    col_ids = jnp.arange(GENES, dtype=jnp.int32)[None, :]
    level_exp = jax.random.randint(subkeys[0], (1, GENES), 0, 2)
    gene_level = jnp.left_shift(jnp.int32(1), level_exp) * (12 * col_ids // GENES + 1)
    cell_level = jax.random.randint(subkeys[1], (CELLS, 1), 1, 4) * (6 * row_ids // CELLS + 2)
    ceiling = (gene_level * cell_level + 15) // 16
    background = jax.random.randint(subkeys[2], (CELLS, GENES), 0, ceiling + 1)
    marker = (col_ids == row_ids % GENES).astype(jnp.int32)
    rolled = jax.random.randint(subkeys[3], (CELLS, GENES), 0, 6400 * GENES)
    spikes = jnp.where(rolled < 400, 200 + rolled, 0)
    return (background + marker + spikes).astype(jnp.int32)


def block_scale(rng, extent, pieces, low, high):
    loudness = 1.0
    for position, shards_of in pieces:
        steps = jax.random.uniform(jax.random.fold_in(jax.random.fold_in(rng, 6), position), (shards_of,), jnp.float32, low / len(pieces), high / len(pieces))
        loudness = loudness * jnp.repeat(jnp.exp(steps), extent[position] // shards_of).reshape((-1,) + (1,) * (len(extent) - 1 - position))
    return loudness


def centred(key, extent, scale, most, cuts=(), kind=jnp.bfloat16):
    values = scale * jax.random.normal(key, extent, jnp.float32)
    if cuts:
        values = values * block_scale(key, extent, cuts, -0.22, 0.18)
    return jnp.clip(values, -most, most).astype(kind)


def setup_inputs(seed: int = 0) -> dict:
    key_list = jax.random.split(jax.random.key(seed), 3)
    return {
        "counts": draw_counts(jax.random.fold_in(key_list[2], 71), 0),
        "sketch": centred(key_list[1], (GENES, RANK), 1.0, 6.0, ((0, 4),)),
    }


def residual_block(block, cell_total, frac, limit):
    values = block.astype(jnp.float32)
    expected = cell_total[:, None] * frac[None, :]
    scaled = (values - expected) / jnp.sqrt(expected + 0.01 * expected * expected)
    return jnp.clip(scaled, -limit, limit).astype(jnp.bfloat16)

def self_gram(block):
    return lax.dot_general(block.astype(jnp.float32), block.astype(jnp.float32), (((0,), (0,)), ((), ())), precision=lax.Precision.HIGHEST, preferred_element_type=jnp.float32)

def whitening(gram, count):
    width = gram.shape[0]
    identity = jnp.eye(width, dtype=jnp.float32)
    shifted = gram + 1e-05 * jnp.trace(gram) / width * identity
    lower = jnp.linalg.cholesky(shifted)
    inverse = jax.scipy.linalg.solve_triangular(lower, identity, lower=True)
    return jnp.transpose(inverse) * math.sqrt(count)

def reference(counts, sketch):
    cell_total = lax.optimization_barrier(jnp.sum(counts, axis=1)).astype(jnp.float32)
    gene_total = lax.optimization_barrier(jnp.sum(counts, axis=0)).astype(jnp.float32)
    grand = jnp.sum(gene_total)
    frac = gene_total / grand
    limit = math.sqrt(float(CELLS))
    blocks = counts.reshape(N_CELLS, CELL_DEV, GENES)
    cell_blocks = cell_total.reshape(N_CELLS, CELL_DEV)
    gene_scale = math.sqrt(float(GENES)) / float(CELLS)
    omega = sketch
    basis = None
    loadings = None
    for sweep in range(ITERS):

        def sketch_block(operands, omega=omega):
            resid = residual_block(operands[0], operands[1], frac, limit)
            return jnp.dot(resid.astype(jnp.float32), omega.astype(jnp.float32), preferred_element_type=jnp.float32)
        sketched = lax.map(sketch_block, (blocks, cell_blocks)).reshape(CELLS, RANK)
        basis = jnp.dot(sketched, whitening(self_gram(sketched), float(CELLS)), precision=lax.Precision.HIGHEST)
        basis_blocks = basis.astype(jnp.bfloat16).reshape(N_CELLS, CELL_DEV, RANK)

        def add_block(total, operands):
            resid = residual_block(operands[0], operands[1], frac, limit)
            term = lax.dot_general(resid.astype(jnp.float32), operands[2].astype(jnp.float32), (((0,), (0,)), ((), ())), preferred_element_type=jnp.float32)
            return (total + term, None)
        start_total = jnp.zeros((GENES, RANK), jnp.float32)
        summed, _ = lax.scan(add_block, start_total, (blocks, cell_blocks, basis_blocks))
        loadings = summed * gene_scale
        if sweep < ITERS - 1:
            omega = loadings.astype(jnp.bfloat16)
    return (basis, loadings)
```

```python
import functools
import math

import jax
import jax.numpy as jnp
from jax import lax
from jax.experimental import pallas as pl
from jax.experimental.pallas import tpu as pltpu
from jax.sharding import PartitionSpec as P

ITERS = 2
MESH = pl.DeviceIdType.MESH


def greet(peers):
    barrier = pltpu.get_barrier_semaphore()
    for peer in peers:
        pl.semaphore_signal(barrier, inc=1, device_id=peer, device_id_type=MESH)
    pl.semaphore_wait(barrier, len(peers))


def ring_peers(axis, count):
    me = lax.axis_index(axis)
    return [{axis: lax.rem(me + step, count)} for step in range(1, count)]


def send(src, dst, sems, slot, peer):
    copy = pltpu.make_async_remote_copy(
        src_ref=src,
        dst_ref=dst,
        send_sem=sems.at[0, slot],
        recv_sem=sems.at[1, slot],
        device_id=peer,
        device_id_type=MESH,
    )
    copy.start()
    return copy


def sems(count):
    return pltpu.SemaphoreType.DMA((2, max(count, 1)))


def remote_call(body, out_shape, scratch, ident):
    leaves = jax.tree.leaves(out_shape)
    specs = [pl.BlockSpec(memory_space=pltpu.VMEM)] * len(leaves)

    def call(*args):
        return pl.pallas_call(
            body,
            out_shape=out_shape,
            in_specs=[pl.BlockSpec(memory_space=pltpu.VMEM)] * len(args),
            out_specs=specs if isinstance(out_shape, (list, tuple)) else specs[0],
            scratch_shapes=scratch,
            compiler_params=pltpu.CompilerParams(
                collective_id=ident, has_side_effects=True, vmem_limit_bytes=16 * 1024 * 1024
            ),
        )(*args)

    return call


def totals_body(n, m, gene_ref, cell_ref, gene_out, cell_out, grand_out, gene_buf, cell_buf, row, row_buf, gene_sem, cell_sem, row_sem):
    cell_peers = ring_peers("cells", n)
    gene_peers = ring_peers("genes", m)
    greet(cell_peers + gene_peers)
    gene_copies = [send(gene_ref, gene_buf.at[i], gene_sem, i, peer) for i, peer in enumerate(cell_peers)]
    cell_copies = [send(cell_ref, cell_buf.at[i], cell_sem, i, peer) for i, peer in enumerate(gene_peers)]
    total = gene_ref[...]
    for i, copy in enumerate(gene_copies):
        copy.wait_recv()
        total = total + gene_buf[i]
    gene_out[...] = total
    row[...] = jnp.broadcast_to(jnp.sum(total, axis=0, keepdims=True), row.shape)
    row_copies = [send(row, row_buf.at[i], row_sem, i, peer) for i, peer in enumerate(gene_peers)]
    total = cell_ref[...]
    for i, copy in enumerate(cell_copies):
        copy.wait_recv()
        total = total + cell_buf[i]
    cell_out[...] = total
    total = row[...]
    for i, copy in enumerate(row_copies):
        copy.wait_recv()
        total = total + row_buf[i]
    grand_out[...] = total
    for copy in gene_copies + cell_copies + row_copies:
        copy.wait_send()


def all_totals(gene_part, cell_part, n, m, ident):
    f32 = jnp.float32
    return remote_call(
        functools.partial(totals_body, n, m),
        [
            jax.ShapeDtypeStruct(gene_part.shape, f32),
            jax.ShapeDtypeStruct(cell_part.shape, f32),
            jax.ShapeDtypeStruct((8, 128), f32),
        ],
        [
            pltpu.VMEM((n - 1,) + gene_part.shape, f32),
            pltpu.VMEM((m - 1,) + cell_part.shape, f32),
            pltpu.VMEM((8, 128), f32),
            pltpu.VMEM((m - 1, 8, 128), f32),
            sems(n - 1),
            sems(m - 1),
            sems(m - 1),
        ],
        ident,
    )(gene_part, cell_part)


def gene_places(m):
    me = lax.axis_index("genes")
    rows = m // 2
    core, row = lax.rem(me, 2), lax.div(me, 2)
    partner = {"genes": row * 2 + 1 - core}
    others = [lax.rem(row + step, rows) for step in range(1, rows)]
    return core, row, partner, others, [{"genes": other * 2 + core} for other in others]


def scatter_body(m, x_ref, out_ref, near, outgoing, far, near_sem, far_sem):
    core, row, partner, others, peers = gene_places(m)
    greet([partner] + peers)
    first = [send(x_ref.at[1 - core, other], near.at[other], near_sem, i, partner) for i, other in enumerate(others + [row])]
    second = []
    for i, other in enumerate(others):
        first[i].wait_recv()
        outgoing[i] = x_ref[core, other] + near[other]
        second.append(send(outgoing.at[i], far.at[i], far_sem, i, peers[i]))
    first[-1].wait_recv()
    out_ref[...] = x_ref[core, row] + near[row]
    for i, copy in enumerate(second):
        copy.wait_recv()
        out_ref[...] += far[i]
    for copy in first + second:
        copy.wait_send()


def scatter_genes(x, m, ident):
    block = x.shape[0] // m
    rows = m // 2
    f32 = jnp.float32
    return remote_call(
        functools.partial(scatter_body, m),
        jax.ShapeDtypeStruct((block, x.shape[1]), f32),
        [
            pltpu.VMEM((rows, block, x.shape[1]), f32),
            pltpu.VMEM((max(rows - 1, 1), block, x.shape[1]), f32),
            pltpu.VMEM((max(rows - 1, 1), block, x.shape[1]), f32),
            sems(rows),
            sems(rows - 1),
        ],
        ident,
    )(x.reshape(2, rows, block, x.shape[1]))


def gather_body(m, x_ref, out_ref, far_sem, near_sem):
    core, row, partner, others, peers = gene_places(m)
    rows = m // 2
    greet([partner] + peers)
    mine = out_ref.at[core, row]
    out_ref[core, row] = x_ref[...]
    far = [send(x_ref, mine, far_sem, i, peer) for i, peer in enumerate(peers)]
    near = [send(x_ref, mine, near_sem, 0, partner)]
    for i in range(rows - 1):
        far[i].wait_recv()
        origin = lax.rem(row + rows - 1 - i, rows)
        near.append(send(out_ref.at[core, origin], out_ref.at[core, origin], near_sem, i + 1, partner))
    for copy in near:
        copy.wait_recv()
    for copy in far + near:
        copy.wait_send()


def gather_genes(x, m, ident):
    rows = m // 2
    out = remote_call(
        functools.partial(gather_body, m),
        jax.ShapeDtypeStruct((2, rows) + x.shape, x.dtype),
        [sems(rows - 1), sems(rows)],
        ident,
    )(x)
    return out.reshape(m * x.shape[0], x.shape[1])


def gram_body(n, m, x_ref, out_ref, buf, part, part_buf, first_sem, part_sem, last_sem):
    me = lax.axis_index("cells")
    cell_peers = ring_peers("cells", n)
    gene_peers = ring_peers("genes", m)
    greet(cell_peers + gene_peers)
    first = [send(x_ref.at[peer["cells"]], buf.at[i], first_sem, i, peer) for i, peer in enumerate(cell_peers)]
    total = x_ref[me]
    for i, copy in enumerate(first):
        copy.wait_recv()
        total = total + buf[i]
    part[...] = total
    middle = [send(part, part_buf.at[i], part_sem, i, peer) for i, peer in enumerate(gene_peers)]
    for i, copy in enumerate(middle):
        copy.wait_recv()
        total = total + part_buf[i]
    out_ref[me] = total
    last = [send(out_ref.at[me], out_ref.at[me], last_sem, i, peer) for i, peer in enumerate(cell_peers)]
    for copy in last:
        copy.wait_recv()
    for copy in first + middle + last:
        copy.wait_send()


def sum_gram(gram, n, m, ident):
    width = gram.shape[0]
    shape = (n, width // n, width)
    f32 = jnp.float32
    out = remote_call(
        functools.partial(gram_body, n, m),
        jax.ShapeDtypeStruct(shape, f32),
        [
            pltpu.VMEM((n - 1,) + shape[1:], f32),
            pltpu.VMEM(shape[1:], f32),
            pltpu.VMEM((m - 1,) + shape[1:], f32),
            sems(n - 1),
            sems(m - 1),
            sems(n - 1),
        ],
        ident,
    )(gram.reshape(shape))
    return out.reshape(width, width)


def loading_body(n, scale, x_ref, out_ref, buf, first_sem, last_sem):
    me = lax.axis_index("cells")
    peers = ring_peers("cells", n)
    greet(peers)
    first = [send(x_ref.at[peer["cells"]], buf.at[i], first_sem, i, peer) for i, peer in enumerate(peers)]
    total = x_ref[me]
    for i, copy in enumerate(first):
        copy.wait_recv()
        total = total + buf[i]
    out_ref[me] = (total * scale).astype(out_ref.dtype)
    last = [send(out_ref.at[me], out_ref.at[me], last_sem, i, peer) for i, peer in enumerate(peers)]
    for copy in last:
        copy.wait_recv()
    for copy in first + last:
        copy.wait_send()


def loading_total(partial_sum, scale, n, ident):
    genes, width = partial_sum.shape
    unit = 16 * n
    padded = -(-genes // unit) * unit
    shape = (n, padded // n, width)
    x = jnp.pad(partial_sum, ((0, padded - genes), (0, 0))).reshape(shape)
    out = remote_call(
        functools.partial(loading_body, n, scale),
        jax.ShapeDtypeStruct(shape, jnp.bfloat16),
        [pltpu.VMEM((n - 1,) + shape[1:], jnp.float32), sems(n - 1), sems(n - 1)],
        ident,
    )(x)
    return out.reshape(padded, width)[:genes]


def residual_block(block, cell_total, frac, limit):
    values = block.astype(jnp.float32)
    expected = cell_total[:, None] * frac[None, :]
    scaled = (values - expected) / jnp.sqrt(expected + 0.01 * expected * expected)
    return jnp.clip(scaled, -limit, limit).astype(jnp.bfloat16)


def self_gram(block):
    return lax.dot_general(
        block,
        block,
        (((0,), (0,)), ((), ())),
        precision=lax.Precision.HIGHEST,
        preferred_element_type=jnp.float32,
    )


def whitening(gram, count):
    width = gram.shape[0]
    identity = jnp.eye(width, dtype=jnp.float32)
    shifted = gram + 1e-05 * jnp.trace(gram) / width * identity
    lower = jnp.linalg.cholesky(shifted)
    inverse = jax.scipy.linalg.solve_triangular(lower, identity, lower=True)
    return jnp.transpose(inverse) * math.sqrt(count)


def transposed_product(left, right):
    return lax.dot_general(
        left, right, (((0,), (0,)), ((), ())), preferred_element_type=jnp.float32
    )


def as_rows(vector):
    length = vector.shape[0]
    padded = -(-length // 128) * 128
    return jnp.pad(vector, (0, padded - length)).reshape(padded // 128, 128)


def shards(counts, sketch):
    cell_dev, gene_dev = counts.shape
    n, m = lax.axis_size("cells"), lax.axis_size("genes")
    cell_count = float(cell_dev * n)
    gene_count = float(gene_dev * m)
    cell_part = jnp.sum(counts, axis=1).astype(jnp.float32)
    gene_part = jnp.sum(counts, axis=0).astype(jnp.float32)
    gene_rows, cell_rows, grand_rows = all_totals(as_rows(gene_part), as_rows(cell_part), n, m, 0)
    gene_total = gene_rows.reshape(-1)[:gene_dev]
    cell_total = cell_rows.reshape(-1)[:cell_dev]
    frac = gene_total / jnp.sum(grand_rows[0])
    limit = math.sqrt(cell_count)
    resid = residual_block(counts, cell_total, frac, limit)
    gene_scale = math.sqrt(gene_count) / cell_count
    omega = sketch
    basis = None
    for sweep in range(ITERS):
        ident = 1 + 4 * sweep
        part = jnp.dot(resid, omega, preferred_element_type=jnp.float32)
        own = scatter_genes(part, m, ident)
        gram = sum_gram(self_gram(own), n, m, ident + 1)
        own_basis = jnp.dot(own, whitening(gram, cell_count), precision=lax.Precision.HIGHEST)
        basis = gather_genes(own_basis.astype(jnp.bfloat16), m, ident + 2)
        partial_sum = transposed_product(resid, basis)
        omega = loading_total(partial_sum, gene_scale, n, ident + 3)
    return (basis.astype(jnp.float32), omega.astype(jnp.float32))


def solution(mesh):
    return jax.shard_map(
        shards,
        mesh=mesh,
        in_specs=(P("cells", "genes"), P("genes", None)),
        out_specs=(P("cells", None), P("genes", None)),
        check_vma=False,
    )
```

```python
import functools
import math

import jax
import jax.numpy as jnp
from jax import lax
from jax.experimental import pallas as pl
from jax.experimental.pallas import tpu as pltpu
from jax.sharding import PartitionSpec as P

ITERS = 2
MESH = pl.DeviceIdType.MESH


def greet(peers):
    barrier = pltpu.get_barrier_semaphore()
    for peer in peers:
        pl.semaphore_signal(barrier, inc=1, device_id=peer, device_id_type=MESH)
    pl.semaphore_wait(barrier, len(peers))


def ring_peers(axis, count):
    me = lax.axis_index(axis)
    return [{axis: lax.rem(me + step, count)} for step in range(1, count)]


def send(src, dst, sems, slot, peer):
    copy = pltpu.make_async_remote_copy(
        src_ref=src,
        dst_ref=dst,
        send_sem=sems.at[0, slot],
        recv_sem=sems.at[1, slot],
        device_id=peer,
        device_id_type=MESH,
    )
    copy.start()
    return copy


def sems(count):
    return pltpu.SemaphoreType.DMA((2, max(count, 1)))


def remote_call(body, out_shape, scratch, ident):
    leaves = jax.tree.leaves(out_shape)
    specs = [pl.BlockSpec(memory_space=pltpu.VMEM)] * len(leaves)

    def call(*args):
        return pl.pallas_call(
            body,
            out_shape=out_shape,
            in_specs=[pl.BlockSpec(memory_space=pltpu.VMEM)] * len(args),
            out_specs=specs if isinstance(out_shape, (list, tuple)) else specs[0],
            scratch_shapes=scratch,
            compiler_params=pltpu.CompilerParams(
                collective_id=ident, has_side_effects=True, vmem_limit_bytes=16 * 1024 * 1024
            ),
        )(*args)

    return call


def totals_body(n, m, gene_ref, cell_ref, gene_out, cell_out, grand_out, gene_buf, cell_buf, row, row_buf, gene_sem, cell_sem, row_sem):
    cell_peers = ring_peers("cells", n)
    gene_peers = ring_peers("genes", m)
    greet(cell_peers + gene_peers)
    gene_copies = [send(gene_ref, gene_buf.at[i], gene_sem, i, peer) for i, peer in enumerate(cell_peers)]
    cell_copies = [send(cell_ref, cell_buf.at[i], cell_sem, i, peer) for i, peer in enumerate(gene_peers)]
    total = gene_ref[...]
    for i, copy in enumerate(gene_copies):
        copy.wait_recv()
        total = total + gene_buf[i]
    gene_out[...] = total
    row[...] = jnp.broadcast_to(jnp.sum(total, axis=0, keepdims=True), row.shape)
    row_copies = [send(row, row_buf.at[i], row_sem, i, peer) for i, peer in enumerate(gene_peers)]
    total = cell_ref[...]
    for i, copy in enumerate(cell_copies):
        copy.wait_recv()
        total = total + cell_buf[i]
    cell_out[...] = total
    total = row[...]
    for i, copy in enumerate(row_copies):
        copy.wait_recv()
        total = total + row_buf[i]
    grand_out[...] = total
    for copy in gene_copies + cell_copies + row_copies:
        copy.wait_send()


def all_totals(gene_part, cell_part, n, m, ident):
    f32 = jnp.float32
    return remote_call(
        functools.partial(totals_body, n, m),
        [
            jax.ShapeDtypeStruct(gene_part.shape, f32),
            jax.ShapeDtypeStruct(cell_part.shape, f32),
            jax.ShapeDtypeStruct((8, 128), f32),
        ],
        [
            pltpu.VMEM((n - 1,) + gene_part.shape, f32),
            pltpu.VMEM((m - 1,) + cell_part.shape, f32),
            pltpu.VMEM((8, 128), f32),
            pltpu.VMEM((m - 1, 8, 128), f32),
            sems(n - 1),
            sems(m - 1),
            sems(m - 1),
        ],
        ident,
    )(gene_part, cell_part)


def gene_places(m):
    me = lax.axis_index("genes")
    rows = m // 2
    core, row = lax.rem(me, 2), lax.div(me, 2)
    partner = {"genes": row * 2 + 1 - core}
    others = [lax.rem(row + step, rows) for step in range(1, rows)]
    return core, row, partner, others, [{"genes": other * 2 + core} for other in others]


def scatter_body(m, x_ref, out_ref, near, outgoing, far, near_sem, far_sem):
    core, row, partner, others, peers = gene_places(m)
    greet([partner] + peers)
    first = [send(x_ref.at[1 - core, other], near.at[other], near_sem, i, partner) for i, other in enumerate(others + [row])]
    second = []
    for i, other in enumerate(others):
        first[i].wait_recv()
        outgoing[i] = x_ref[core, other] + near[other]
        second.append(send(outgoing.at[i], far.at[i], far_sem, i, peers[i]))
    first[-1].wait_recv()
    out_ref[...] = x_ref[core, row] + near[row]
    for i, copy in enumerate(second):
        copy.wait_recv()
        out_ref[...] += far[i]
    for copy in first + second:
        copy.wait_send()


def scatter_genes(x, m, ident):
    block = x.shape[0] // m
    rows = m // 2
    f32 = jnp.float32
    return remote_call(
        functools.partial(scatter_body, m),
        jax.ShapeDtypeStruct((block, x.shape[1]), f32),
        [
            pltpu.VMEM((rows, block, x.shape[1]), f32),
            pltpu.VMEM((max(rows - 1, 1), block, x.shape[1]), f32),
            pltpu.VMEM((max(rows - 1, 1), block, x.shape[1]), f32),
            sems(rows),
            sems(rows - 1),
        ],
        ident,
    )(x.reshape(2, rows, block, x.shape[1]))


def gather_body(m, x_ref, out_ref, far_sem, near_sem):
    core, row, partner, others, peers = gene_places(m)
    rows = m // 2
    greet([partner] + peers)
    mine = out_ref.at[core, row]
    out_ref[core, row] = x_ref[...]
    far = [send(x_ref, mine, far_sem, i, peer) for i, peer in enumerate(peers)]
    near = [send(x_ref, mine, near_sem, 0, partner)]
    for i in range(rows - 1):
        far[i].wait_recv()
        origin = lax.rem(row + rows - 1 - i, rows)
        near.append(send(out_ref.at[core, origin], out_ref.at[core, origin], near_sem, i + 1, partner))
    for copy in near:
        copy.wait_recv()
    for copy in far + near:
        copy.wait_send()


def gather_genes(x, m, ident):
    rows = m // 2
    out = remote_call(
        functools.partial(gather_body, m),
        jax.ShapeDtypeStruct((2, rows) + x.shape, x.dtype),
        [sems(rows - 1), sems(rows)],
        ident,
    )(x)
    return out.reshape(m * x.shape[0], x.shape[1])


def gram_body(n, m, x_ref, out_ref, buf, part, part_buf, first_sem, part_sem, last_sem):
    me = lax.axis_index("cells")
    cell_peers = ring_peers("cells", n)
    gene_peers = ring_peers("genes", m)
    greet(cell_peers + gene_peers)
    first = [send(x_ref.at[peer["cells"]], buf.at[i], first_sem, i, peer) for i, peer in enumerate(cell_peers)]
    total = x_ref[me]
    for i, copy in enumerate(first):
        copy.wait_recv()
        total = total + buf[i]
    part[...] = total
    middle = [send(part, part_buf.at[i], part_sem, i, peer) for i, peer in enumerate(gene_peers)]
    for i, copy in enumerate(middle):
        copy.wait_recv()
        total = total + part_buf[i]
    out_ref[me] = total
    last = [send(out_ref.at[me], out_ref.at[me], last_sem, i, peer) for i, peer in enumerate(cell_peers)]
    for copy in last:
        copy.wait_recv()
    for copy in first + middle + last:
        copy.wait_send()


def sum_gram(gram, n, m, ident):
    width = gram.shape[0]
    shape = (n, width // n, width)
    f32 = jnp.float32
    out = remote_call(
        functools.partial(gram_body, n, m),
        jax.ShapeDtypeStruct(shape, f32),
        [
            pltpu.VMEM((n - 1,) + shape[1:], f32),
            pltpu.VMEM(shape[1:], f32),
            pltpu.VMEM((m - 1,) + shape[1:], f32),
            sems(n - 1),
            sems(m - 1),
            sems(n - 1),
        ],
        ident,
    )(gram.reshape(shape))
    return out.reshape(width, width)


def loading_body(n, scale, x_ref, out_ref, buf, first_sem, last_sem):
    me = lax.axis_index("cells")
    peers = ring_peers("cells", n)
    greet(peers)
    first = [send(x_ref.at[peer["cells"]], buf.at[i], first_sem, i, peer) for i, peer in enumerate(peers)]
    total = x_ref[me]
    for i, copy in enumerate(first):
        copy.wait_recv()
        total = total + buf[i]
    out_ref[me] = (total * scale).astype(out_ref.dtype)
    last = [send(out_ref.at[me], out_ref.at[me], last_sem, i, peer) for i, peer in enumerate(peers)]
    for copy in last:
        copy.wait_recv()
    for copy in first + last:
        copy.wait_send()


def loading_total(partial_sum, scale, n, ident):
    genes, width = partial_sum.shape
    unit = 16 * n
    padded = -(-genes // unit) * unit
    shape = (n, padded // n, width)
    x = jnp.pad(partial_sum, ((0, padded - genes), (0, 0))).reshape(shape)
    out = remote_call(
        functools.partial(loading_body, n, scale),
        jax.ShapeDtypeStruct(shape, jnp.bfloat16),
        [pltpu.VMEM((n - 1,) + shape[1:], jnp.float32), sems(n - 1), sems(n - 1)],
        ident,
    )(x)
    return out.reshape(padded, width)[:genes]


def residual_block(block, cell_total, frac, limit):
    values = block.astype(jnp.float32)
    expected = cell_total[:, None] * frac[None, :]
    scaled = (values - expected) / jnp.sqrt(expected + 0.01 * expected * expected)
    return jnp.clip(scaled, -limit, limit).astype(jnp.bfloat16)


def self_gram(block):
    return lax.dot_general(
        block,
        block,
        (((0,), (0,)), ((), ())),
        precision=lax.Precision.HIGHEST,
        preferred_element_type=jnp.float32,
    )


def whiten_body(scale, gram_ref, out_ref, left, right):
    width = gram_ref.shape[0]
    eye = lax.broadcasted_iota(jnp.int32, (width, width), 0) == lax.broadcasted_iota(jnp.int32, (width, width), 1)
    gram = gram_ref[...]
    diagonal = jnp.where(eye, gram, 0.0)
    trace = jnp.sum(jnp.sum(diagonal, axis=1, keepdims=True), axis=0, keepdims=True)
    left[...] = gram + jnp.where(eye, 1e-05 * trace / width, 0.0)
    right[...] = jnp.where(eye, 1.0, 0.0)
    place = lax.broadcasted_iota(jnp.int32, (8, width), 0)
    contract = functools.partial(
        lax.dot_general,
        dimension_numbers=(((0,), (0,)), ((), ())),
        precision=lax.Precision.HIGHEST,
        preferred_element_type=jnp.float32,
    )

    def panel(step, carry):
        rows_left, rows_right = left[:8, :], right[:8, :]
        columns = [jnp.broadcast_to(rows_left[:, i : i + 1], (8, width)) for i in range(8)]
        done_left = jnp.zeros((8, width), jnp.float32)
        done_right = jnp.zeros((8, width), jnp.float32)
        for i in range(8):
            inverse = lax.rsqrt(columns[i][i : i + 1, :])
            top_left, top_right = rows_left[i : i + 1, :] * inverse, rows_right[i : i + 1, :] * inverse
            done_left = jnp.where(place == i, top_left, done_left)
            done_right = jnp.where(place == i, top_right, done_right)
            if i < 7:
                factor = jnp.where(place > i, columns[i] * inverse, 0.0)
                rows_left = rows_left - factor * top_left
                rows_right = rows_right - factor * top_right
                for j in range(i + 1, 8):
                    columns[j] = columns[j] - factor * (columns[j][i : i + 1, :] * inverse)
        out_ref[pl.ds(pl.multiple_of(step * 8, 8), 8), :] = done_right * scale
        new_left = pltpu.roll(left[...] - contract(done_left, done_left), width - 8, 1)
        new_right = right[...] - contract(done_left, done_right)
        left[: width - 8, :] = new_left[8:, :]
        right[: width - 8, :] = new_right[8:, :]
        left[width - 8 :, :] = jnp.zeros((8, width), jnp.float32)
        right[width - 8 :, :] = jnp.zeros((8, width), jnp.float32)
        return carry

    lax.fori_loop(0, width // 8, panel, 0)


def whitening(gram, count):
    shape = jax.ShapeDtypeStruct(gram.shape, jnp.float32)
    return pl.pallas_call(
        functools.partial(whiten_body, math.sqrt(count)),
        out_shape=shape,
        in_specs=[pl.BlockSpec(memory_space=pltpu.VMEM)],
        out_specs=pl.BlockSpec(memory_space=pltpu.VMEM),
        scratch_shapes=[pltpu.VMEM(gram.shape, jnp.float32)] * 2,
        compiler_params=pltpu.CompilerParams(vmem_limit_bytes=16 * 1024 * 1024),
    )(gram)


def transposed_product(left, right):
    return lax.dot_general(
        left, right, (((0,), (0,)), ((), ())), preferred_element_type=jnp.float32
    )


def as_rows(vector):
    length = vector.shape[0]
    padded = -(-length // 128) * 128
    return jnp.pad(vector, (0, padded - length)).reshape(padded // 128, 128)


def shards(counts, sketch):
    cell_dev, gene_dev = counts.shape
    n, m = lax.axis_size("cells"), lax.axis_size("genes")
    cell_count = float(cell_dev * n)
    gene_count = float(gene_dev * m)
    cell_part = jnp.sum(counts, axis=1).astype(jnp.float32)
    gene_part = jnp.sum(counts, axis=0).astype(jnp.float32)
    gene_rows, cell_rows, grand_rows = all_totals(as_rows(gene_part), as_rows(cell_part), n, m, 0)
    gene_total = gene_rows.reshape(-1)[:gene_dev]
    cell_total = cell_rows.reshape(-1)[:cell_dev]
    frac = gene_total / jnp.sum(grand_rows[0])
    limit = math.sqrt(cell_count)
    resid = residual_block(counts, cell_total, frac, limit)
    gene_scale = math.sqrt(gene_count) / cell_count
    omega = sketch
    basis = None
    for sweep in range(ITERS):
        ident = 1 + 4 * sweep
        part = jnp.dot(resid, omega, preferred_element_type=jnp.float32)
        own = scatter_genes(part, m, ident)
        gram = sum_gram(self_gram(own), n, m, ident + 1)
        own_basis = lax.dot_general(
            own,
            whitening(gram, cell_count),
            (((1,), (1,)), ((), ())),
            precision=lax.Precision.HIGHEST,
            preferred_element_type=jnp.float32,
        )
        basis = gather_genes(own_basis.astype(jnp.bfloat16), m, ident + 2)
        partial_sum = transposed_product(resid, basis)
        omega = loading_total(partial_sum, gene_scale, n, ident + 3)
    return (basis.astype(jnp.float32), omega.astype(jnp.float32))


def solution(mesh):
    return jax.shard_map(
        shards,
        mesh=mesh,
        in_specs=(P("cells", "genes"), P("genes", None)),
        out_specs=(P("cells", None), P("genes", None)),
        check_vma=False,
    )
```
